32 devices in a mesh: cp: 8 (over z, core), fsdp: 4 (over y, x).
Axes of the slice: x: 2, y: 2, z: 4, core: 2. Of those that a mesh axis runs over, the one named last changes fastest.
Arguments:
- tokens: bfloat16 [4, 16, 64, 2304], P('fsdp', 'cp'), may hold values from -6 to 6
- gains: float32 [4, 2304], replicated, may hold values from 0.25 to 1.75
- w_query: bfloat16 [2304, 2048], P(('cp', 'fsdp')), may hold values from -0.125 to 0.125
- w_key: bfloat16 [2304, 1024], P(('cp', 'fsdp')), may hold values from -0.125 to 0.125
- w_value: bfloat16 [2304, 1024], P(('cp', 'fsdp')), may hold values from -0.125 to 0.125
- w_out: bfloat16 [2304, 2048], P(('cp', 'fsdp')), may hold values from -0.125 to 0.125
- w_gate: bfloat16 [2304, 9216], P(('cp', 'fsdp')), may hold values from -0.125 to 0.125
- w_up: bfloat16 [2304, 9216], P(('cp', 'fsdp')), may hold values from -0.125 to 0.125
- w_down: bfloat16 [2304, 9216], P(('cp', 'fsdp')), may hold values from -0.0625 to 0.0625
- order: int32 [16], replicated, may hold values from 0 to 15, as said below
- cotangent: bfloat16 [4, 16, 64, 2304], P('fsdp', 'cp'), may hold values from -6 to 6
Outputs:
- output: bfloat16 [4, 16, 64, 2304], P('fsdp', 'cp')
- grad_tokens: float32 [4, 16, 64, 2304], P('fsdp', 'cp')
- grad_gains: float32 [4, 2304], P(None, ('cp', 'fsdp'))
- grad_query: float32 [2304, 2048], P(('cp', 'fsdp'))
- grad_key: float32 [2304, 1024], P(('cp', 'fsdp'))
- grad_value: float32 [2304, 1024], P(('cp', 'fsdp'))
- grad_out: float32 [2304, 2048], P(('cp', 'fsdp'))
- grad_gate: float32 [2304, 9216], P(('cp', 'fsdp'))
- grad_up: float32 [2304, 9216], P(('cp', 'fsdp'))
- grad_down: float32 [2304, 9216], P(('cp', 'fsdp'))
The draws below stay inside these ranges and needn't reach their ends.
Inputs may be any that keep to these rules, and one draw needn't show every extreme that they name: order is a permutation of the causal block numbers; stored blocks 2c and 2c + 1 hold two blocks whose numbers add up to 15, in either order.
All inputs are finite; a program needn't handle non-finite values.
Results may differ from the reference program's by a relative error of at most 0.022.
Values may be sent and summed in bfloat16 or wider, within the bound.
A program may use at most 320 MiB of HBM per device.

```python
import math
import jax
import jax.numpy as jnp
from jax import lax

D = 2304
HEADS = 8
KV_HEADS = 4
HEAD = 256
FF = 9216
SPAN = 64
SLOTS = 16
LENGTH = 1024
BATCH = 4


def draw_order(key, part):
    pair_count = SLOTS // 2
    early_spans = jax.random.permutation(jax.random.fold_in(key, 11), pair_count).astype(jnp.int32)
    flipped = jax.random.randint(jax.random.fold_in(key, 12), (pair_count,), 0, 2, dtype=jnp.int32)
    late_spans = SLOTS - 1 - early_spans
    first_slot = jnp.where(flipped == 1, late_spans, early_spans)
    second_slot = jnp.where(flipped == 1, early_spans, late_spans)
    return jnp.stack([first_slot, second_slot], axis=1).reshape(SLOTS).astype(jnp.int32)


def strengthened(entries, key, source, target, blocks, factor):
    owner, partner = [(jnp.arange(entries.shape[axis_at]) // (entries.shape[axis_at] // blocks)).reshape([-1 if axis == axis_at else 1 for axis in range(entries.ndim)]) for axis_at in (source, target)]
    chosen = jax.random.permutation(key, blocks)[partner]
    strong = (owner == chosen) | (owner == (partner + blocks // 2) % blocks)
    return jnp.where(strong, factor * entries, entries)


def level_of(rng, dims, split, least, high):
    level = 1.0
    for position, blocks in split:
        draws = jax.random.uniform(jax.random.fold_in(jax.random.fold_in(rng, 6), position), (blocks,), jnp.float32, least / len(split), high / len(split))
        level = level * jnp.repeat(jnp.exp(draws), dims[position] // blocks).reshape((-1,) + (1,) * (len(dims) - 1 - position))
    return level


def noise(key, dims, spread, limit, split=(), held_as=jnp.bfloat16):
    drawn = jax.random.normal(key, dims, jnp.float32) * spread
    if len(split) > 0:
        drawn = level_of(key, dims, split, -0.22, 0.18) * drawn
    return jnp.clip(drawn, min=-limit, max=limit).astype(held_as)


def gaussian_with(rng, shape, width, reach, split, heavy, kind=jnp.bfloat16):
    drawn = width * jax.random.normal(rng, shape, jnp.float32)
    if split:
        drawn = drawn * level_of(rng, shape, split, -0.22, 0.18)
    return jnp.clip(strengthened(drawn, jax.random.fold_in(rng, 3), *heavy), -reach, reach).astype(kind)


def setup_inputs(seed: int = 0) -> dict:
    arg_keys = jax.random.split(jax.random.key(seed), 12)
    tokens = noise(arg_keys[0], (BATCH, SLOTS, SPAN, D), 1.0, 6.0, ((0, 4), (1, 8)))
    gains = jnp.clip(1.0 + 0.15 * jax.random.normal(arg_keys[1], (4, D), jnp.float32), 0.25, 1.75)
    w_query = noise(arg_keys[2], (D, HEADS * HEAD), D ** -0.5, 0.125, ((0, 32),))
    w_key = noise(arg_keys[3], (D, KV_HEADS * HEAD), D ** -0.5, 0.125, ((0, 32),))
    w_value = noise(arg_keys[4], (D, KV_HEADS * HEAD), D ** -0.5, 0.125, ((0, 32),))
    w_out = noise(arg_keys[5], (D, HEADS * HEAD), (HEADS * HEAD) ** -0.5, 0.125, ((0, 32),))
    w_gate = noise(arg_keys[6], (D, FF), D ** -0.5, 0.125, ((0, 32),))
    w_up = noise(arg_keys[7], (D, FF), D ** -0.5, 0.125, ((0, 32),))
    w_down = noise(arg_keys[8], (D, FF), FF ** -0.5, 0.0625, ((0, 32),))
    order = draw_order(jax.random.fold_in(arg_keys[11], 71), 0)
    cotangent = gaussian_with(arg_keys[10], (BATCH, SLOTS, SPAN, D), 1.0, 6.0, ((0, 4), (1, 8)), (1, 3, 8, 2.0))
    return dict(tokens=tokens, gains=gains, w_query=w_query, w_key=w_key, w_value=w_value, w_out=w_out, w_gate=w_gate, w_up=w_up, w_down=w_down, order=order, cotangent=cotangent)


@jax.custom_vjp
def low(v):
    return lax.optimization_barrier(v.astype(jnp.bfloat16)).astype(jnp.float32)

@jax.custom_vjp
def low_back(v):
    return v

def low_keep(v):
    return (low(v), None)

def low_pass(kept, grad):
    return (grad,)

def back_keep(v):
    return (v, None)

def back_low(kept, grad):
    return (low(grad),)
low.defvjp(low_keep, low_pass)
low_back.defvjp(back_keep, back_low)
SOFT_CAP = 50.0
NORM_EPS = 1e-06
ROPE_BASE = 10000.0
HIGHEST = lax.Precision.HIGHEST

def normalize(values):
    return values * lax.rsqrt(lax.optimization_barrier(jnp.mean(values * values, axis=-1, keepdims=True)) + NORM_EPS)

def rotary(values, cosine, sine):
    middle = values.shape[-1] // 2
    first = values[..., :middle]
    second = values[..., middle:]
    cos_b = cosine[:, None, :]
    sin_b = sine[:, None, :]
    return jnp.concatenate([first * cos_b - second * sin_b, second * cos_b + first * sin_b], axis=-1)

def reference(tokens, gains, w_query, w_key, w_value, w_out, w_gate, w_up, w_down, order, cotangent):
    groups = HEADS // KV_HEADS
    scale_q = HEAD ** (-0.5)
    offsets = jnp.arange(SPAN, dtype=jnp.int32)
    positions = (order.astype(jnp.int32)[:, None] * SPAN + offsets[None, :]).reshape(-1)
    visible = positions[None, :] <= positions[:, None]
    inverse = jnp.exp(-math.log(ROPE_BASE) * jnp.arange(HEAD // 2, dtype=jnp.float32) * 2.0 / HEAD)
    angle = positions.astype(jnp.float32)[:, None] * inverse[None, :]
    cosine = jnp.cos(angle)
    sine = jnp.sin(angle)

    def attend(triple):
        query, keys, values = triple
        grouped = query.reshape(LENGTH, KV_HEADS, groups, HEAD)
        raw = low_back(jnp.einsum('tkgd,skd->kgts', grouped, keys, precision=HIGHEST) * scale_q)
        scores = jnp.where(visible, SOFT_CAP * jnp.tanh(raw / SOFT_CAP), -1e+30)
        probs = low(jax.nn.softmax(scores, axis=-1))
        mixed = jnp.einsum('kgts,skd->tkgd', probs, values, precision=HIGHEST)
        return mixed.reshape(LENGTH, HEADS * HEAD)

    def forward(hidden, gain_rows, wq, wk, wv, wo, wg, wu, wd):
        attn_in = low(normalize(hidden) * gain_rows[0])
        q_lin = low_back(jnp.einsum('bld,de->ble', attn_in, wq, precision=HIGHEST))
        k_lin = low_back(jnp.einsum('bld,de->ble', attn_in, wk, precision=HIGHEST))
        v_lin = low_back(jnp.einsum('bld,de->ble', attn_in, wv, precision=HIGHEST))
        rot = jax.vmap(rotary, in_axes=(0, None, None))
        query = low(rot(q_lin.reshape(BATCH, LENGTH, HEADS, HEAD), cosine, sine))
        keys = low(rot(k_lin.reshape(BATCH, LENGTH, KV_HEADS, HEAD), cosine, sine))
        values = low(v_lin.reshape(BATCH, LENGTH, KV_HEADS, HEAD))
        attended = lax.map(jax.checkpoint(attend), (query, keys, values))
        attended = low(low_back(attended))
        attn_out = low_back(jnp.einsum('blc,dc->bld', attended, wo, precision=HIGHEST))
        mid = hidden + normalize(attn_out) * gain_rows[1]
        ffn_in = low(normalize(mid) * gain_rows[2])
        gate = low_back(jnp.einsum('bld,df->blf', ffn_in, wg, precision=HIGHEST))
        upper = low_back(jnp.einsum('bld,df->blf', ffn_in, wu, precision=HIGHEST))
        inner = low(jax.nn.gelu(gate, approximate=True) * upper)
        ffn_out = low_back(jnp.einsum('blf,df->bld', inner, wd, precision=HIGHEST))
        return mid + normalize(ffn_out) * gain_rows[3]
    hidden = tokens.astype(jnp.float32).reshape(BATCH, LENGTH, D)
    weights = [w.astype(jnp.float32) for w in (w_query, w_key, w_value, w_out, w_gate, w_up, w_down)]
    result, backward = jax.vjp(forward, hidden, gains.astype(jnp.float32), *weights)
    grads = backward(cotangent.astype(jnp.float32).reshape(BATCH, LENGTH, D))
    output = result.astype(jnp.bfloat16).reshape(BATCH, SLOTS, SPAN, D)
    grad_tokens = grads[0].reshape(BATCH, SLOTS, SPAN, D)
    return (output, grad_tokens, grads[1], grads[2], grads[3], grads[4], grads[5], grads[6], grads[7], grads[8])
```

```python
from functools import partial
import math

import jax
import jax.numpy as jnp
from jax import lax
from jax.sharding import PartitionSpec as P

HEADS = 8
KV_HEADS = 4
HEAD = 256


SOFT_CAP = 50.0
NORM_EPS = 1e-06
ROPE_BASE = 10000.0
CONTRACT_LAST = (((1,), (1,)), ((), ()))
CONTRACT_FIRST = (((0,), (0,)), ((), ()))


def normalize(values):
    factor = lax.rsqrt(jnp.mean(values * values, axis=-1, keepdims=True) + NORM_EPS)
    return (values * factor, factor)


def norm_back(grad_normed, normed, factor):
    return factor * (grad_normed - normed * jnp.mean(grad_normed * normed, axis=-1, keepdims=True))


def rotary(values, cosine, sine, direction):
    middle = values.shape[-1] // 2
    first = values[..., :middle]
    second = values[..., middle:]
    cos_b = cosine[:, None, :]
    sin_b = sine[:, None, :] * direction
    return jnp.concatenate(
        [first * cos_b - second * sin_b, second * cos_b + first * sin_b], axis=-1
    )


def local(tokens, gains, w_query, w_key, w_value, w_out, w_gate, w_up, w_down, order, cotangent):
    width = tokens.shape[-1]
    span = tokens.shape[2]
    q_width = w_query.shape[1]
    kv_width = w_key.shape[1]
    groups = HEADS // KV_HEADS
    scale_q = HEAD ** (-0.5)
    context = lax.axis_index("cp")
    local_order = lax.dynamic_slice_in_dim(order, 2 * context, 2)
    offsets = jnp.arange(span, dtype=jnp.int32)
    local_pos = (local_order[:, None] * span + offsets[None, :]).reshape(-1)
    every_pos = (order[:, None] * span + offsets[None, :]).reshape(-1)
    visible = every_pos[None, :] <= local_pos[:, None]
    inverse = jnp.exp(-math.log(ROPE_BASE) * jnp.arange(HEAD // 2, dtype=jnp.float32) * 2.0 / HEAD)
    angle = local_pos.astype(jnp.float32)[:, None] * inverse[None, :]
    cosine = jnp.cos(angle)
    sine = jnp.sin(angle)
    hidden = tokens.reshape(-1, width).astype(jnp.float32)
    count_rows = hidden.shape[0]
    normed_one, factor_one = normalize(hidden)
    attn_in = (normed_one * gains[0]).astype(jnp.bfloat16)
    pieces = (
        lax.all_gather(w_query, ("cp", "fsdp"), axis=0, tiled=True),
        lax.all_gather(w_key, ("cp", "fsdp"), axis=0, tiled=True),
        lax.all_gather(w_value, ("cp", "fsdp"), axis=0, tiled=True),
    )
    columns = attn_in
    q_lin, k_lin, v_lin = tuple(
        (jnp.dot(columns, piece, preferred_element_type=jnp.float32) for piece in pieces)
    )
    query_low = rotary(q_lin.reshape(count_rows, HEADS, HEAD), cosine, sine, 1.0).astype(
        jnp.bfloat16
    )
    key_low = rotary(k_lin.reshape(count_rows, KV_HEADS, HEAD), cosine, sine, 1.0).astype(
        jnp.bfloat16
    )
    value_low = v_lin.astype(jnp.bfloat16)
    query_groups = query_low.reshape(count_rows, KV_HEADS, groups, HEAD)

    def share_keys():
        blocks = (
            lax.all_gather(key_low.reshape(2, span, kv_width), "cp", axis=0, tiled=True),
            lax.all_gather(value_low.reshape(2, span, kv_width), "cp", axis=0, tiled=True),
        )
        return (blocks[0].reshape(-1, KV_HEADS, HEAD), blocks[1].reshape(-1, KV_HEADS, HEAD))

    def bent_scores(keys_all):
        raw = (
            jnp.einsum("tkgd,skd->kgts", query_groups, keys_all, preferred_element_type=jnp.float32)
            * scale_q
        )
        return jnp.tanh(raw / SOFT_CAP)

    keys_all, values_all = share_keys()
    bent = bent_scores(keys_all)
    scores = jnp.where(visible, SOFT_CAP * bent, -1e30)
    top_score = jnp.max(scores, axis=-1, keepdims=True)
    expo = jnp.exp(scores - top_score)
    total_mass = jnp.sum(expo, axis=-1, keepdims=True)
    log_total = top_score + jnp.log(total_mass)
    probs_low = (expo / total_mass).astype(jnp.bfloat16)
    attended = jnp.einsum(
        "kgts,skd->tkgd", probs_low, values_all, preferred_element_type=jnp.float32
    )
    attended_low = attended.reshape(count_rows, q_width).astype(jnp.bfloat16)
    attn_out = lax.dot_general(
        attended_low,
        lax.all_gather(w_out, ("cp", "fsdp"), axis=0, tiled=True),
        CONTRACT_LAST,
        preferred_element_type=jnp.float32,
    )
    normed_two, factor_two = normalize(attn_out)
    middle_sum = hidden + normed_two * gains[1]
    normed_three, factor_three = normalize(middle_sum)
    ffn_in = (normed_three * gains[2]).astype(jnp.bfloat16)
    relayed = (
        lax.all_to_all(w_gate, "fsdp", split_axis=1, concat_axis=0, tiled=True),
        lax.all_to_all(w_up, "fsdp", split_axis=1, concat_axis=0, tiled=True),
        lax.all_to_all(w_down, "fsdp", split_axis=1, concat_axis=0, tiled=True),
    )
    gate_part, up_part, down_part = (
        lax.all_gather(relayed[0], "cp", axis=0, tiled=True),
        lax.all_gather(relayed[1], "cp", axis=0, tiled=True),
        lax.all_gather(relayed[2], "cp", axis=0, tiled=True),
    )
    group_in = lax.all_gather(ffn_in, "fsdp", axis=0, tiled=True)
    gate = jnp.dot(group_in, gate_part, preferred_element_type=jnp.float32)
    upper = jnp.dot(group_in, up_part, preferred_element_type=jnp.float32)
    activated = jax.nn.gelu(gate, approximate=True)
    inner_low = (activated * upper).astype(jnp.bfloat16)
    share_out = lax.dot_general(
        inner_low, down_part, CONTRACT_LAST, preferred_element_type=jnp.float32
    )
    ffn_out = lax.psum_scatter(
        share_out.astype(jnp.bfloat16), "fsdp", scatter_dimension=0, tiled=True
    ).astype(jnp.float32)
    normed_four, factor_four = normalize(ffn_out)
    result = middle_sum + normed_four * gains[3]
    output = result.astype(jnp.bfloat16).reshape(tokens.shape)
    grad_result = cotangent.reshape(-1, width).astype(jnp.float32)
    gain_four = jnp.sum(grad_result * normed_four, axis=0)
    grad_ffn_low = norm_back(grad_result * gains[3], normed_four, factor_four).astype(jnp.bfloat16)
    group_grad = lax.all_gather(grad_ffn_low, "fsdp", axis=0, tiled=True)
    grad_inner = jnp.dot(group_grad, down_part, preferred_element_type=jnp.float32)
    unused_value, gelu_back = jax.vjp(partial(jax.nn.gelu, approximate=True), gate)
    grad_gate_low = gelu_back(grad_inner * upper)[0].astype(jnp.bfloat16)
    grad_upper_low = (grad_inner * activated).astype(jnp.bfloat16)
    share_in = lax.dot_general(
        grad_gate_low, gate_part, CONTRACT_LAST, preferred_element_type=jnp.float32
    ) + lax.dot_general(grad_upper_low, up_part, CONTRACT_LAST, preferred_element_type=jnp.float32)
    grad_ffn_in = lax.psum_scatter(
        share_in.astype(jnp.bfloat16), "fsdp", scatter_dimension=0, tiled=True
    ).astype(jnp.float32)
    part_width = gate_part.shape[1]
    slice_sums = lax.psum_scatter(
        jnp.concatenate(
            [
                lax.dot_general(
                    group_in, grad_gate_low, CONTRACT_FIRST, preferred_element_type=jnp.float32
                ),
                lax.dot_general(
                    group_in, grad_upper_low, CONTRACT_FIRST, preferred_element_type=jnp.float32
                ),
                lax.dot_general(
                    group_grad, inner_low, CONTRACT_FIRST, preferred_element_type=jnp.float32
                ),
            ],
            axis=1,
        ).astype(jnp.bfloat16),
        "cp",
        scatter_dimension=0,
        tiled=True,
    ).astype(jnp.float32)
    grad_gate, grad_up, grad_down = (
        lax.all_to_all(
            slice_sums[:, :part_width].astype(jnp.bfloat16),
            "fsdp",
            split_axis=0,
            concat_axis=1,
            tiled=True,
        ).astype(jnp.float32),
        lax.all_to_all(
            slice_sums[:, part_width : 2 * part_width].astype(jnp.bfloat16),
            "fsdp",
            split_axis=0,
            concat_axis=1,
            tiled=True,
        ).astype(jnp.float32),
        lax.all_to_all(
            slice_sums[:, 2 * part_width :].astype(jnp.bfloat16),
            "fsdp",
            split_axis=0,
            concat_axis=1,
            tiled=True,
        ).astype(jnp.float32),
    )
    gain_three = jnp.sum(grad_ffn_in * normed_three, axis=0)
    grad_middle = grad_result + norm_back(grad_ffn_in * gains[2], normed_three, factor_three)
    gain_two = jnp.sum(grad_middle * normed_two, axis=0)
    grad_attn_low = norm_back(grad_middle * gains[1], normed_two, factor_two).astype(jnp.bfloat16)
    columns = grad_attn_low
    grad_attended = jnp.dot(
        columns,
        lax.all_gather(w_out, ("cp", "fsdp"), axis=0, tiled=True),
        preferred_element_type=jnp.float32,
    )
    grad_att_low = grad_attended.astype(jnp.bfloat16).reshape(count_rows, KV_HEADS, groups, HEAD)
    keys_back, values_back = share_keys()
    bent_back = bent_scores(keys_back)
    probs_full = jnp.where(visible, jnp.exp(SOFT_CAP * bent_back - log_total), 0.0)
    probs_back = probs_full.astype(jnp.bfloat16)
    grad_probs = jnp.einsum(
        "tkgd,skd->kgts", grad_att_low, values_back, preferred_element_type=jnp.float32
    )
    delta = jnp.sum(grad_probs * probs_full, axis=-1, keepdims=True)
    grad_raw = (probs_full * (grad_probs - delta) * (1.0 - bent_back * bent_back)).astype(
        jnp.bfloat16
    )
    grad_query_rot = (
        jnp.einsum("kgts,skd->tkgd", grad_raw, keys_back, preferred_element_type=jnp.float32)
        * scale_q
    )
    grad_keys_all = (
        jnp.einsum("kgts,tkgd->skd", grad_raw, query_groups, preferred_element_type=jnp.float32)
        * scale_q
    )
    grad_values_all = jnp.einsum(
        "kgts,tkgd->skd", probs_back, grad_att_low, preferred_element_type=jnp.float32
    )
    slots = order.shape[0]
    grad_keys, grad_values = (
        lax.psum_scatter(
            grad_keys_all.reshape(slots, span, kv_width).astype(jnp.bfloat16),
            "cp",
            scatter_dimension=0,
            tiled=True,
        ).astype(jnp.float32),
        lax.psum_scatter(
            grad_values_all.reshape(slots, span, kv_width).astype(jnp.bfloat16),
            "cp",
            scatter_dimension=0,
            tiled=True,
        ).astype(jnp.float32),
    )
    grad_q_low = (
        rotary(grad_query_rot.reshape(count_rows, HEADS, HEAD), cosine, sine, -1.0)
        .reshape(count_rows, q_width)
        .astype(jnp.bfloat16)
    )
    grad_k_low = (
        rotary(grad_keys.reshape(count_rows, KV_HEADS, HEAD), cosine, sine, -1.0)
        .reshape(count_rows, kv_width)
        .astype(jnp.bfloat16)
    )
    grad_v_low = grad_values.reshape(count_rows, kv_width).astype(jnp.bfloat16)
    pieces = lax.all_gather((w_query, w_key, w_value), ("cp", "fsdp"), axis=0, tiled=True)
    grad_attn_in = (
        lax.dot_general(grad_q_low, pieces[0], CONTRACT_LAST, preferred_element_type=jnp.float32)
        + lax.dot_general(grad_k_low, pieces[1], CONTRACT_LAST, preferred_element_type=jnp.float32)
        + lax.dot_general(grad_v_low, pieces[2], CONTRACT_LAST, preferred_element_type=jnp.float32)
    )
    gain_one = jnp.sum(grad_attn_in * normed_one, axis=0)
    grad_hidden = grad_middle + norm_back(grad_attn_in * gains[0], normed_one, factor_one)
    gain_columns = jnp.stack([gain_one, gain_two, gain_three, gain_four], axis=1)
    attn_terms = jnp.concatenate(
        [
            lax.dot_general(
                attn_in, grad_q_low, CONTRACT_FIRST, preferred_element_type=jnp.float32
            ),
            lax.dot_general(
                attn_in, grad_k_low, CONTRACT_FIRST, preferred_element_type=jnp.float32
            ),
            lax.dot_general(
                attn_in, grad_v_low, CONTRACT_FIRST, preferred_element_type=jnp.float32
            ),
            lax.dot_general(
                grad_attn_low, attended_low, CONTRACT_FIRST, preferred_element_type=jnp.float32
            ),
            gain_columns,
        ],
        axis=1,
    )
    attn_sums = lax.psum_scatter(attn_terms, ("cp", "fsdp"), scatter_dimension=0, tiled=True)
    grad_query = attn_sums[:, :q_width]
    grad_key = attn_sums[:, q_width : q_width + kv_width]
    grad_value = attn_sums[:, q_width + kv_width : q_width + 2 * kv_width]
    grad_out = attn_sums[:, q_width + 2 * kv_width : 2 * q_width + 2 * kv_width]
    grad_gains = attn_sums[:, 2 * q_width + 2 * kv_width :].T
    return (
        output,
        grad_hidden.reshape(tokens.shape),
        grad_gains,
        grad_query,
        grad_key,
        grad_value,
        grad_out,
        grad_gate,
        grad_up,
        grad_down,
    )


def weights_in(shard):
    pieces = lax.all_to_all(shard, "cp", split_axis=1, concat_axis=0, tiled=False)
    rows, ranks, columns = shard.shape
    whole = lax.all_gather(pieces.reshape(-1, columns), "fsdp", axis=0, tiled=True)
    whole = whole.reshape(-1, ranks, rows, columns).transpose(1, 0, 2, 3)
    return whole.reshape(-1, columns)


def weights_out(grads, ranks, planes):
    rows = grads.shape[0] // (ranks * planes)
    parted = grads.astype(jnp.bfloat16).reshape(ranks, planes, rows, grads.shape[1])
    parted = parted.transpose(1, 0, 2, 3).reshape(grads.shape)
    sums = lax.psum_scatter(parted, "fsdp", scatter_dimension=0, tiled=True)
    return lax.all_to_all(
        sums.reshape(ranks, rows, -1), "cp", split_axis=0, concat_axis=1, tiled=False
    )


def by_heads(
    tokens, gains, w_query, w_key, w_value, w_out, w_gate, w_up, w_down, order, cotangent
):
    width = tokens.shape[-1]
    span = tokens.shape[2]
    rows = w_query.shape[0]
    ranks = lax.axis_size("cp")
    planes = lax.axis_size("fsdp")
    scale_q = HEAD ** (-0.5)
    rank = lax.axis_index("cp")
    even = rank % 2 == 0
    offsets = jnp.arange(span, dtype=jnp.int32)
    positions = (order[:, None] * span + offsets[None, :]).reshape(-1)
    visible = positions[None, :] <= positions[:, None]
    inverse = jnp.exp(-math.log(ROPE_BASE) * jnp.arange(HEAD // 2, dtype=jnp.float32) * 2.0 / HEAD)
    angle = positions.astype(jnp.float32)[:, None] * inverse[None, :]
    cosine = jnp.cos(angle)
    sine = jnp.sin(angle)
    mixed_cos = jnp.where(even, cosine, 1.0)
    mixed_sin = jnp.where(even, sine, 0.0)

    def turn(values, cos_t, sin_t):
        middle = values.shape[-1] // 2
        first = values[:, :middle]
        second = values[:, middle:]
        return jnp.concatenate(
            [first * cos_t - second * sin_t, second * cos_t + first * sin_t], axis=-1
        )

    swap = [(i, i ^ 1) for i in range(ranks)]
    hidden = tokens.reshape(-1, width).astype(jnp.float32)
    normed_one, factor_one = normalize(hidden)
    attn_in = (normed_one * gains[0]).astype(jnp.bfloat16)
    seq_in = lax.all_gather(attn_in, "cp", axis=0, tiled=True)
    pairs = jnp.stack(
        [w_key.reshape(rows, KV_HEADS, HEAD), w_value.reshape(rows, KV_HEADS, HEAD)], axis=2
    ).reshape(rows, ranks, HEAD)
    attn_w = weights_in(
        jnp.concatenate(
            [w_query.reshape(rows, ranks, HEAD), pairs, w_out.reshape(rows, ranks, HEAD)], axis=-1
        )
    )
    w_lin = attn_w[:, : 2 * HEAD]
    w_back = attn_w[:, 2 * HEAD :]
    lin = jnp.dot(seq_in, w_lin, preferred_element_type=jnp.float32)
    query = turn(lin[:, :HEAD], cosine, sine).astype(jnp.bfloat16)
    mixed = turn(lin[:, HEAD:], mixed_cos, mixed_sin).astype(jnp.bfloat16)
    other = lax.ppermute(mixed, "cp", swap)
    keys = jnp.where(even, mixed, other)
    values = jnp.where(even, other, mixed)
    raw = lax.dot_general(query, keys, CONTRACT_LAST, preferred_element_type=jnp.float32) * scale_q
    bent = jnp.tanh(raw / SOFT_CAP)
    scores = jnp.where(visible, SOFT_CAP * bent, -1e30)
    top_score = jnp.max(scores, axis=-1, keepdims=True)
    expo = jnp.exp(scores - top_score)
    total_mass = jnp.sum(expo, axis=-1, keepdims=True)
    probs_full = expo / total_mass
    probs_low = probs_full.astype(jnp.bfloat16)
    attended_low = jnp.dot(probs_low, values, preferred_element_type=jnp.float32).astype(
        jnp.bfloat16
    )
    share_attn = lax.dot_general(
        attended_low, w_back, CONTRACT_LAST, preferred_element_type=jnp.float32
    )
    attn_out = lax.psum_scatter(
        share_attn.astype(jnp.bfloat16), "cp", scatter_dimension=0, tiled=True
    ).astype(jnp.float32)
    normed_two, factor_two = normalize(attn_out)
    middle_sum = hidden + normed_two * gains[1]
    normed_three, factor_three = normalize(middle_sum)
    ffn_in = (normed_three * gains[2]).astype(jnp.bfloat16)
    gate_part, up_part, down_part = (
        weights_in(piece.reshape(rows, ranks, -1)) for piece in (w_gate, w_up, w_down)
    )
    group_in = lax.all_gather(ffn_in, "cp", axis=0, tiled=True)
    gate = jnp.dot(group_in, gate_part, preferred_element_type=jnp.float32)
    upper = jnp.dot(group_in, up_part, preferred_element_type=jnp.float32)
    activated = jax.nn.gelu(gate, approximate=True)
    inner_low = (activated * upper).astype(jnp.bfloat16)
    share_out = lax.dot_general(
        inner_low, down_part, CONTRACT_LAST, preferred_element_type=jnp.float32
    )
    ffn_out = lax.psum_scatter(
        share_out.astype(jnp.bfloat16), "cp", scatter_dimension=0, tiled=True
    ).astype(jnp.float32)
    normed_four, factor_four = normalize(ffn_out)
    result = middle_sum + normed_four * gains[3]
    output = result.astype(jnp.bfloat16).reshape(tokens.shape)
    grad_result = cotangent.reshape(-1, width).astype(jnp.float32)
    gain_four = jnp.sum(grad_result * normed_four, axis=0)
    grad_ffn_low = norm_back(grad_result * gains[3], normed_four, factor_four).astype(jnp.bfloat16)
    group_grad = lax.all_gather(grad_ffn_low, "cp", axis=0, tiled=True)
    grad_inner = jnp.dot(group_grad, down_part, preferred_element_type=jnp.float32)
    unused_value, gelu_back = jax.vjp(partial(jax.nn.gelu, approximate=True), gate)
    grad_gate_low = gelu_back(grad_inner * upper)[0].astype(jnp.bfloat16)
    grad_upper_low = (grad_inner * activated).astype(jnp.bfloat16)
    share_in = lax.dot_general(
        grad_gate_low, gate_part, CONTRACT_LAST, preferred_element_type=jnp.float32
    ) + lax.dot_general(grad_upper_low, up_part, CONTRACT_LAST, preferred_element_type=jnp.float32)
    grad_ffn_in = lax.psum_scatter(
        share_in.astype(jnp.bfloat16), "cp", scatter_dimension=0, tiled=True
    ).astype(jnp.float32)
    grad_gate, grad_up, grad_down = (
        weights_out(
            lax.dot_general(left, right, CONTRACT_FIRST, preferred_element_type=jnp.float32),
            ranks,
            planes,
        )
        .astype(jnp.float32)
        .reshape(rows, -1)
        for left, right in (
            (group_in, grad_gate_low),
            (group_in, grad_upper_low),
            (group_grad, inner_low),
        )
    )
    gain_three = jnp.sum(grad_ffn_in * normed_three, axis=0)
    grad_middle = grad_result + norm_back(grad_ffn_in * gains[2], normed_three, factor_three)
    gain_two = jnp.sum(grad_middle * normed_two, axis=0)
    grad_attn_low = norm_back(grad_middle * gains[1], normed_two, factor_two).astype(jnp.bfloat16)
    seq_grad = lax.all_gather(grad_attn_low, "cp", axis=0, tiled=True)
    grad_att_low = jnp.dot(seq_grad, w_back, preferred_element_type=jnp.float32).astype(
        jnp.bfloat16
    )
    grad_probs = lax.dot_general(
        grad_att_low, values, CONTRACT_LAST, preferred_element_type=jnp.float32
    )
    delta = jnp.sum(grad_probs * probs_full, axis=-1, keepdims=True)
    grad_raw = (probs_full * (grad_probs - delta) * (1.0 - bent * bent)).astype(jnp.bfloat16)
    grad_query = jnp.dot(grad_raw, keys, preferred_element_type=jnp.float32) * scale_q
    grad_keys = (
        lax.dot_general(grad_raw, query, CONTRACT_FIRST, preferred_element_type=jnp.float32)
        * scale_q
    )
    grad_values = lax.dot_general(
        probs_low, grad_att_low, CONTRACT_FIRST, preferred_element_type=jnp.float32
    )
    grad_mixed = jnp.where(even, grad_keys, grad_values) + lax.ppermute(
        jnp.where(even, grad_values, grad_keys), "cp", swap
    )
    grad_lin = jnp.concatenate(
        [
            turn(grad_query, cosine, -sine).astype(jnp.bfloat16),
            turn(grad_mixed, mixed_cos, -mixed_sin).astype(jnp.bfloat16),
        ],
        axis=1,
    )
    share_back = lax.dot_general(
        grad_lin, w_lin, CONTRACT_LAST, preferred_element_type=jnp.float32
    )
    grad_attn_in = lax.psum_scatter(
        share_back.astype(jnp.bfloat16), "cp", scatter_dimension=0, tiled=True
    ).astype(jnp.float32)
    attn_sums = weights_out(
        jnp.concatenate(
            [
                lax.dot_general(
                    seq_in, grad_lin, CONTRACT_FIRST, preferred_element_type=jnp.float32
                ),
                lax.dot_general(
                    seq_grad, attended_low, CONTRACT_FIRST, preferred_element_type=jnp.float32
                ),
            ],
            axis=1,
        ),
        ranks,
        planes,
    ).astype(jnp.float32)
    grad_wq = attn_sums[:, :, :HEAD].reshape(rows, -1)
    grad_pairs = attn_sums[:, :, HEAD : 2 * HEAD].reshape(rows, KV_HEADS, 2, HEAD)
    grad_wk = grad_pairs[:, :, 0].reshape(rows, -1)
    grad_wv = grad_pairs[:, :, 1].reshape(rows, -1)
    grad_wo = attn_sums[:, :, 2 * HEAD :].reshape(rows, -1)
    gain_one = jnp.sum(grad_attn_in * normed_one, axis=0)
    grad_hidden = grad_middle + norm_back(grad_attn_in * gains[0], normed_one, factor_one)
    gain_columns = jnp.stack([gain_one, gain_two, gain_three, gain_four], axis=1)
    grad_gains = lax.psum_scatter(
        gain_columns, ("cp", "fsdp"), scatter_dimension=0, tiled=True
    ).T
    return (
        output,
        grad_hidden.reshape(tokens.shape),
        grad_gains,
        grad_wq,
        grad_wk,
        grad_wv,
        grad_wo,
        grad_gate,
        grad_up,
        grad_down,
    )


def solution(mesh):
    return jax.shard_map(
        by_heads if mesh.shape["cp"] == HEADS else local,
        mesh=mesh,
        in_specs=(
            P("fsdp", "cp", None, None),
            P(),
            P(("cp", "fsdp"), None),
            P(("cp", "fsdp"), None),
            P(("cp", "fsdp"), None),
            P(("cp", "fsdp"), None),
            P(("cp", "fsdp"), None),
            P(("cp", "fsdp"), None),
            P(("cp", "fsdp"), None),
            P(),
            P("fsdp", "cp", None, None),
        ),
        out_specs=(
            P("fsdp", "cp", None, None),
            P("fsdp", "cp", None, None),
            P(None, ("cp", "fsdp")),
            P(("cp", "fsdp"), None),
            P(("cp", "fsdp"), None),
            P(("cp", "fsdp"), None),
            P(("cp", "fsdp"), None),
            P(("cp", "fsdp"), None),
            P(("cp", "fsdp"), None),
            P(("cp", "fsdp"), None),
        ),
        check_vma=False,
    )
```

```python
from functools import partial
import math

import jax
import jax.numpy as jnp
from jax import lax
from jax.experimental import pallas as pl
from jax.experimental.pallas import tpu as pltpu
from jax.sharding import PartitionSpec as P

HEADS = 8
KV_HEADS = 4
HEAD = 256


SOFT_CAP = 50.0
NORM_EPS = 1e-06
ROPE_BASE = 10000.0
CONTRACT_LAST = (((1,), (1,)), ((), ()))
CONTRACT_FIRST = (((0,), (0,)), ((), ()))


def normalize(values):
    factor = lax.rsqrt(jnp.mean(values * values, axis=-1, keepdims=True) + NORM_EPS)
    return (values * factor, factor)


def norm_back(grad_normed, normed, factor):
    return factor * (grad_normed - normed * jnp.mean(grad_normed * normed, axis=-1, keepdims=True))


def rotary(values, cosine, sine, direction):
    middle = values.shape[-1] // 2
    first = values[..., :middle]
    second = values[..., middle:]
    cos_b = cosine[:, None, :]
    sin_b = sine[:, None, :] * direction
    return jnp.concatenate(
        [first * cos_b - second * sin_b, second * cos_b + first * sin_b], axis=-1
    )


def local(tokens, gains, w_query, w_key, w_value, w_out, w_gate, w_up, w_down, order, cotangent):
    width = tokens.shape[-1]
    span = tokens.shape[2]
    q_width = w_query.shape[1]
    kv_width = w_key.shape[1]
    groups = HEADS // KV_HEADS
    scale_q = HEAD ** (-0.5)
    context = lax.axis_index("cp")
    local_order = lax.dynamic_slice_in_dim(order, 2 * context, 2)
    offsets = jnp.arange(span, dtype=jnp.int32)
    local_pos = (local_order[:, None] * span + offsets[None, :]).reshape(-1)
    every_pos = (order[:, None] * span + offsets[None, :]).reshape(-1)
    visible = every_pos[None, :] <= local_pos[:, None]
    inverse = jnp.exp(-math.log(ROPE_BASE) * jnp.arange(HEAD // 2, dtype=jnp.float32) * 2.0 / HEAD)
    angle = local_pos.astype(jnp.float32)[:, None] * inverse[None, :]
    cosine = jnp.cos(angle)
    sine = jnp.sin(angle)
    hidden = tokens.reshape(-1, width).astype(jnp.float32)
    count_rows = hidden.shape[0]
    normed_one, factor_one = normalize(hidden)
    attn_in = (normed_one * gains[0]).astype(jnp.bfloat16)
    pieces = (
        lax.all_gather(w_query, ("cp", "fsdp"), axis=0, tiled=True),
        lax.all_gather(w_key, ("cp", "fsdp"), axis=0, tiled=True),
        lax.all_gather(w_value, ("cp", "fsdp"), axis=0, tiled=True),
    )
    columns = attn_in
    q_lin, k_lin, v_lin = tuple(
        (jnp.dot(columns, piece, preferred_element_type=jnp.float32) for piece in pieces)
    )
    query_low = rotary(q_lin.reshape(count_rows, HEADS, HEAD), cosine, sine, 1.0).astype(
        jnp.bfloat16
    )
    key_low = rotary(k_lin.reshape(count_rows, KV_HEADS, HEAD), cosine, sine, 1.0).astype(
        jnp.bfloat16
    )
    value_low = v_lin.astype(jnp.bfloat16)
    query_groups = query_low.reshape(count_rows, KV_HEADS, groups, HEAD)

    def share_keys():
        blocks = (
            lax.all_gather(key_low.reshape(2, span, kv_width), "cp", axis=0, tiled=True),
            lax.all_gather(value_low.reshape(2, span, kv_width), "cp", axis=0, tiled=True),
        )
        return (blocks[0].reshape(-1, KV_HEADS, HEAD), blocks[1].reshape(-1, KV_HEADS, HEAD))

    def bent_scores(keys_all):
        raw = (
            jnp.einsum("tkgd,skd->kgts", query_groups, keys_all, preferred_element_type=jnp.float32)
            * scale_q
        )
        return jnp.tanh(raw / SOFT_CAP)

    keys_all, values_all = share_keys()
    bent = bent_scores(keys_all)
    scores = jnp.where(visible, SOFT_CAP * bent, -1e30)
    top_score = jnp.max(scores, axis=-1, keepdims=True)
    expo = jnp.exp(scores - top_score)
    total_mass = jnp.sum(expo, axis=-1, keepdims=True)
    log_total = top_score + jnp.log(total_mass)
    probs_low = (expo / total_mass).astype(jnp.bfloat16)
    attended = jnp.einsum(
        "kgts,skd->tkgd", probs_low, values_all, preferred_element_type=jnp.float32
    )
    attended_low = attended.reshape(count_rows, q_width).astype(jnp.bfloat16)
    attn_out = lax.dot_general(
        attended_low,
        lax.all_gather(w_out, ("cp", "fsdp"), axis=0, tiled=True),
        CONTRACT_LAST,
        preferred_element_type=jnp.float32,
    )
    normed_two, factor_two = normalize(attn_out)
    middle_sum = hidden + normed_two * gains[1]
    normed_three, factor_three = normalize(middle_sum)
    ffn_in = (normed_three * gains[2]).astype(jnp.bfloat16)
    relayed = (
        lax.all_to_all(w_gate, "fsdp", split_axis=1, concat_axis=0, tiled=True),
        lax.all_to_all(w_up, "fsdp", split_axis=1, concat_axis=0, tiled=True),
        lax.all_to_all(w_down, "fsdp", split_axis=1, concat_axis=0, tiled=True),
    )
    gate_part, up_part, down_part = (
        lax.all_gather(relayed[0], "cp", axis=0, tiled=True),
        lax.all_gather(relayed[1], "cp", axis=0, tiled=True),
        lax.all_gather(relayed[2], "cp", axis=0, tiled=True),
    )
    group_in = lax.all_gather(ffn_in, "fsdp", axis=0, tiled=True)
    gate = jnp.dot(group_in, gate_part, preferred_element_type=jnp.float32)
    upper = jnp.dot(group_in, up_part, preferred_element_type=jnp.float32)
    activated = jax.nn.gelu(gate, approximate=True)
    inner_low = (activated * upper).astype(jnp.bfloat16)
    share_out = lax.dot_general(
        inner_low, down_part, CONTRACT_LAST, preferred_element_type=jnp.float32
    )
    ffn_out = lax.psum_scatter(
        share_out.astype(jnp.bfloat16), "fsdp", scatter_dimension=0, tiled=True
    ).astype(jnp.float32)
    normed_four, factor_four = normalize(ffn_out)
    result = middle_sum + normed_four * gains[3]
    output = result.astype(jnp.bfloat16).reshape(tokens.shape)
    grad_result = cotangent.reshape(-1, width).astype(jnp.float32)
    gain_four = jnp.sum(grad_result * normed_four, axis=0)
    grad_ffn_low = norm_back(grad_result * gains[3], normed_four, factor_four).astype(jnp.bfloat16)
    group_grad = lax.all_gather(grad_ffn_low, "fsdp", axis=0, tiled=True)
    grad_inner = jnp.dot(group_grad, down_part, preferred_element_type=jnp.float32)
    unused_value, gelu_back = jax.vjp(partial(jax.nn.gelu, approximate=True), gate)
    grad_gate_low = gelu_back(grad_inner * upper)[0].astype(jnp.bfloat16)
    grad_upper_low = (grad_inner * activated).astype(jnp.bfloat16)
    share_in = lax.dot_general(
        grad_gate_low, gate_part, CONTRACT_LAST, preferred_element_type=jnp.float32
    ) + lax.dot_general(grad_upper_low, up_part, CONTRACT_LAST, preferred_element_type=jnp.float32)
    grad_ffn_in = lax.psum_scatter(
        share_in.astype(jnp.bfloat16), "fsdp", scatter_dimension=0, tiled=True
    ).astype(jnp.float32)
    part_width = gate_part.shape[1]
    slice_sums = lax.psum_scatter(
        jnp.concatenate(
            [
                lax.dot_general(
                    group_in, grad_gate_low, CONTRACT_FIRST, preferred_element_type=jnp.float32
                ),
                lax.dot_general(
                    group_in, grad_upper_low, CONTRACT_FIRST, preferred_element_type=jnp.float32
                ),
                lax.dot_general(
                    group_grad, inner_low, CONTRACT_FIRST, preferred_element_type=jnp.float32
                ),
            ],
            axis=1,
        ).astype(jnp.bfloat16),
        "cp",
        scatter_dimension=0,
        tiled=True,
    ).astype(jnp.float32)
    grad_gate, grad_up, grad_down = (
        lax.all_to_all(
            slice_sums[:, :part_width].astype(jnp.bfloat16),
            "fsdp",
            split_axis=0,
            concat_axis=1,
            tiled=True,
        ).astype(jnp.float32),
        lax.all_to_all(
            slice_sums[:, part_width : 2 * part_width].astype(jnp.bfloat16),
            "fsdp",
            split_axis=0,
            concat_axis=1,
            tiled=True,
        ).astype(jnp.float32),
        lax.all_to_all(
            slice_sums[:, 2 * part_width :].astype(jnp.bfloat16),
            "fsdp",
            split_axis=0,
            concat_axis=1,
            tiled=True,
        ).astype(jnp.float32),
    )
    gain_three = jnp.sum(grad_ffn_in * normed_three, axis=0)
    grad_middle = grad_result + norm_back(grad_ffn_in * gains[2], normed_three, factor_three)
    gain_two = jnp.sum(grad_middle * normed_two, axis=0)
    grad_attn_low = norm_back(grad_middle * gains[1], normed_two, factor_two).astype(jnp.bfloat16)
    columns = grad_attn_low
    grad_attended = jnp.dot(
        columns,
        lax.all_gather(w_out, ("cp", "fsdp"), axis=0, tiled=True),
        preferred_element_type=jnp.float32,
    )
    grad_att_low = grad_attended.astype(jnp.bfloat16).reshape(count_rows, KV_HEADS, groups, HEAD)
    keys_back, values_back = share_keys()
    bent_back = bent_scores(keys_back)
    probs_full = jnp.where(visible, jnp.exp(SOFT_CAP * bent_back - log_total), 0.0)
    probs_back = probs_full.astype(jnp.bfloat16)
    grad_probs = jnp.einsum(
        "tkgd,skd->kgts", grad_att_low, values_back, preferred_element_type=jnp.float32
    )
    delta = jnp.sum(grad_probs * probs_full, axis=-1, keepdims=True)
    grad_raw = (probs_full * (grad_probs - delta) * (1.0 - bent_back * bent_back)).astype(
        jnp.bfloat16
    )
    grad_query_rot = (
        jnp.einsum("kgts,skd->tkgd", grad_raw, keys_back, preferred_element_type=jnp.float32)
        * scale_q
    )
    grad_keys_all = (
        jnp.einsum("kgts,tkgd->skd", grad_raw, query_groups, preferred_element_type=jnp.float32)
        * scale_q
    )
    grad_values_all = jnp.einsum(
        "kgts,tkgd->skd", probs_back, grad_att_low, preferred_element_type=jnp.float32
    )
    slots = order.shape[0]
    grad_keys, grad_values = (
        lax.psum_scatter(
            grad_keys_all.reshape(slots, span, kv_width).astype(jnp.bfloat16),
            "cp",
            scatter_dimension=0,
            tiled=True,
        ).astype(jnp.float32),
        lax.psum_scatter(
            grad_values_all.reshape(slots, span, kv_width).astype(jnp.bfloat16),
            "cp",
            scatter_dimension=0,
            tiled=True,
        ).astype(jnp.float32),
    )
    grad_q_low = (
        rotary(grad_query_rot.reshape(count_rows, HEADS, HEAD), cosine, sine, -1.0)
        .reshape(count_rows, q_width)
        .astype(jnp.bfloat16)
    )
    grad_k_low = (
        rotary(grad_keys.reshape(count_rows, KV_HEADS, HEAD), cosine, sine, -1.0)
        .reshape(count_rows, kv_width)
        .astype(jnp.bfloat16)
    )
    grad_v_low = grad_values.reshape(count_rows, kv_width).astype(jnp.bfloat16)
    pieces = lax.all_gather((w_query, w_key, w_value), ("cp", "fsdp"), axis=0, tiled=True)
    grad_attn_in = (
        lax.dot_general(grad_q_low, pieces[0], CONTRACT_LAST, preferred_element_type=jnp.float32)
        + lax.dot_general(grad_k_low, pieces[1], CONTRACT_LAST, preferred_element_type=jnp.float32)
        + lax.dot_general(grad_v_low, pieces[2], CONTRACT_LAST, preferred_element_type=jnp.float32)
    )
    gain_one = jnp.sum(grad_attn_in * normed_one, axis=0)
    grad_hidden = grad_middle + norm_back(grad_attn_in * gains[0], normed_one, factor_one)
    gain_columns = jnp.stack([gain_one, gain_two, gain_three, gain_four], axis=1)
    attn_terms = jnp.concatenate(
        [
            lax.dot_general(
                attn_in, grad_q_low, CONTRACT_FIRST, preferred_element_type=jnp.float32
            ),
            lax.dot_general(
                attn_in, grad_k_low, CONTRACT_FIRST, preferred_element_type=jnp.float32
            ),
            lax.dot_general(
                attn_in, grad_v_low, CONTRACT_FIRST, preferred_element_type=jnp.float32
            ),
            lax.dot_general(
                grad_attn_low, attended_low, CONTRACT_FIRST, preferred_element_type=jnp.float32
            ),
            gain_columns,
        ],
        axis=1,
    )
    attn_sums = lax.psum_scatter(attn_terms, ("cp", "fsdp"), scatter_dimension=0, tiled=True)
    grad_query = attn_sums[:, :q_width]
    grad_key = attn_sums[:, q_width : q_width + kv_width]
    grad_value = attn_sums[:, q_width + kv_width : q_width + 2 * kv_width]
    grad_out = attn_sums[:, q_width + 2 * kv_width : 2 * q_width + 2 * kv_width]
    grad_gains = attn_sums[:, 2 * q_width + 2 * kv_width :].T
    return (
        output,
        grad_hidden.reshape(tokens.shape),
        grad_gains,
        grad_query,
        grad_key,
        grad_value,
        grad_out,
        grad_gate,
        grad_up,
        grad_down,
    )


MESH_IDS = pl.DeviceIdType.MESH
DMA = pltpu.SemaphoreType.DMA


def remote(source, target, send, recv, **ids):
    return pltpu.make_async_remote_copy(
        src_ref=source,
        dst_ref=target,
        send_sem=send,
        recv_sem=recv,
        device_id=ids,
        device_id_type=MESH_IDS,
    )


class Place:
    def __init__(self, ranks):
        self.ranks = ranks
        self.depth = ranks // 2
        self.rank = lax.axis_index("cp")
        self.plane = lax.axis_index("fsdp")
        self.z = self.rank // 2
        self.core = lax.rem(self.rank, 2)
        self.twin = 2 * self.z + 1 - self.core
        self.above = self.z < self.depth - 1
        self.below = self.z > 0

    def greet(self, column, planes):
        barrier = pltpu.get_barrier_semaphore()

        def signal(**ids):
            pl.semaphore_signal(barrier, inc=1, device_id=ids, device_id_type=MESH_IDS)

        count = 0
        if column:
            for step in range(1, self.ranks):
                signal(cp=lax.rem(self.rank + step, self.ranks))
            count = self.ranks - 1
        else:
            signal(cp=self.twin)

            @pl.when(self.above)
            def _():
                signal(cp=self.rank + 2)

            @pl.when(self.below)
            def _():
                signal(cp=self.rank - 2)

            count = (
                1
                + jnp.where(self.above, 1, 0).astype(jnp.int32)
                + jnp.where(self.below, 1, 0).astype(jnp.int32)
            )
        if planes:
            for flip in (1, 2):
                signal(fsdp=jnp.bitwise_xor(self.plane, flip))
            count = count + 2
        pl.semaphore_wait(barrier, count)


class Gather:
    @staticmethod
    def scratch(ranks):
        return [DMA((3, ranks)), DMA((3, ranks)), DMA]

    def __init__(self, place, source, whole, send, recv, local):
        self.place, self.source, self.whole = place, source, whole
        self.send, self.recv, self.local = send, recv, local

    def copy(self, source, shard, way, step):
        place = self.place
        target = (place.rank + 2, place.rank - 2, place.twin)[way]
        return remote(
            source, self.whole.at[shard], self.send.at[way, step], self.recv.at[way, step], cp=target
        )

    def start(self):
        place = self.place
        pltpu.make_async_copy(self.source, self.whole.at[place.rank], self.local).start()

        @pl.when(place.above)
        def _():
            self.copy(self.source, place.rank, 0, 0).start()

        @pl.when(place.below)
        def _():
            self.copy(self.source, place.rank, 1, 0).start()

        self.copy(self.source, place.rank, 2, 0).start()

    def relay(self, step):
        place = self.place
        last = place.depth - 1

        @pl.when(place.z >= step)
        def _():
            shard = place.rank - 2 * step
            self.copy(self.whole.at[shard], shard, 0, step - 1).wait_recv()

            @pl.when(place.above)
            def _():
                self.copy(self.whole.at[shard], shard, 0, step).start()

            self.copy(self.whole.at[shard], shard, 2, step).start()

        @pl.when(place.z + step <= last)
        def _():
            shard = place.rank + 2 * step
            self.copy(self.whole.at[shard], shard, 1, step - 1).wait_recv()

            @pl.when(place.below)
            def _():
                self.copy(self.whole.at[shard], shard, 1, step).start()

            self.copy(self.whole.at[shard], shard, 2, last + step).start()

    def finish(self):
        place = self.place
        last = place.depth - 1
        own = self.whole.at[place.rank]
        for step in range(place.depth):

            @pl.when(jnp.logical_and(place.z >= step, place.above))
            def _():
                self.copy(own, place.rank, 0, step).wait_send()

            @pl.when(jnp.logical_and(place.z + step <= last, place.below))
            def _():
                self.copy(own, place.rank, 1, step).wait_send()

            @pl.when(place.z >= step)
            def _():
                self.copy(own, place.rank, 2, step).wait()

            if step > 0:

                @pl.when(place.z + step <= last)
                def _():
                    self.copy(own, place.rank, 2, last + step).wait()

        pltpu.make_async_copy(self.source, own, self.local).wait()


class Scatter:
    @staticmethod
    def scratch(ranks, rows, width):
        depth = ranks // 2
        slots = pltpu.VMEM((depth, rows, width), jnp.bfloat16)
        return [slots] * 4 + [DMA((3, depth)), DMA((3, depth))]

    def __init__(self, place, parts, out, pair, rising, falling, outbox, send, recv):
        self.place, self.parts, self.out = place, parts, out
        self.pair, self.rising, self.falling, self.outbox = pair, rising, falling, outbox
        self.send, self.recv = send, recv
        rows = parts.shape[1]
        self.tile = 16
        self.tiles = rows // self.tile

    def swap(self, target):
        place = self.place
        return remote(
            self.parts.at[2 * target + 1 - place.core],
            self.pair.at[target],
            self.send.at[0, target],
            self.recv.at[0, target],
            cp=place.twin,
        )

    def hop(self, target, way):
        box = (self.rising, self.falling)[way]
        return remote(
            self.outbox.at[target],
            box.at[target],
            self.send.at[1 + way, target],
            self.recv.at[1 + way, target],
            cp=self.place.rank + (2, -2)[way],
        )

    def start(self):
        depth = self.place.depth
        for target in sorted(range(depth), key=lambda i: -abs(2 * i - depth + 1)):
            self.swap(target).start()

    def add(self, target, boxes, store):
        place = self.place

        def body(tile, carry):
            rows = pl.ds(pl.multiple_of(tile * self.tile, self.tile), self.tile)
            total = self.parts[2 * target + place.core, rows].astype(jnp.float32) + self.pair[
                target, rows
            ].astype(jnp.float32)
            for box in boxes:
                total = total + box[target, rows].astype(jnp.float32)
            store(rows, total)
            return carry

        lax.fori_loop(0, self.tiles, body, 0)

    def run(self):
        place = self.place

        def send(target, way, fed):
            self.swap(target).wait_recv()
            box = (self.rising, self.falling)[way]

            def store(rows, total):
                self.outbox[target, rows] = total.astype(jnp.bfloat16)

            @pl.when(fed)
            def _():
                self.hop(target, way).wait_recv()
                self.add(target, [box], store)

            @pl.when(jnp.logical_not(fed))
            def _():
                self.add(target, [], store)

            self.hop(target, way).start()

        for step in range(place.depth - 1, 0, -1):

            @pl.when(place.z + step < place.depth)
            def _():
                send(place.z + step, 0, place.below)

            @pl.when(place.z >= step)
            def _():
                send(place.z - step, 1, place.above)

    def finish(self):
        place = self.place
        self.swap(place.z).wait_recv()

        def store(rows, total):
            self.out[rows] = total

        def both():
            self.hop(place.z, 0).wait_recv()
            self.hop(place.z, 1).wait_recv()
            self.add(place.z, [self.rising, self.falling], store)

        def lower():
            self.hop(place.z, 0).wait_recv()
            self.add(place.z, [self.rising], store)

        def upper():
            self.hop(place.z, 1).wait_recv()
            self.add(place.z, [self.falling], store)

        pl.when(jnp.logical_and(place.below, place.above))(both)
        pl.when(jnp.logical_and(place.below, jnp.logical_not(place.above)))(lower)
        pl.when(jnp.logical_and(jnp.logical_not(place.below), place.above))(upper)
        for target in range(place.depth):
            self.swap(target).wait_send()

            @pl.when(target > place.z)
            def _():
                self.hop(target, 0).wait_send()

            @pl.when(target < place.z)
            def _():
                self.hop(target, 1).wait_send()


class Exchange:
    @staticmethod
    def scratch(ranks, rows, columns):
        return [
            pltpu.VMEM((rows, columns), jnp.bfloat16),
            DMA((ranks,)),
            DMA((ranks,)),
            DMA((4,)),
            DMA((4,)),
        ]

    def __init__(self, place, shard, whole, bounce, send, recv, send_plane, recv_plane):
        self.place, self.shard, self.whole, self.bounce = place, shard, whole, bounce
        self.send, self.recv = send, recv
        self.send_plane, self.recv_plane = send_plane, recv_plane
        self.columns = whole.shape[3]
        self.half = place.ranks // 2

    def slice_of(self, target):
        first = pl.multiple_of(target * self.columns, 128)
        return self.shard.at[:, pl.ds(first, self.columns)]

    def piece(self, step):
        place = self.place
        target = lax.rem(place.rank + step, place.ranks)
        return remote(
            self.slice_of(target),
            self.whole.at[place.rank, place.plane],
            self.send.at[step],
            self.recv.at[step],
            cp=target,
        )

    def own(self, inward):
        place = self.place
        if inward:
            return pltpu.make_async_copy(self.slice_of(place.rank), self.bounce, self.send.at[0])
        return pltpu.make_async_copy(
            self.bounce, self.whole.at[place.rank, place.plane], self.recv.at[0]
        )

    def start(self):
        for step in range(1, self.place.ranks):
            self.piece(step).start()
        self.own(True).start()
        self.own(True).wait()
        self.own(False).start()

    def first(self, flip):
        column = self.whole.at[:, self.place.plane]
        return remote(
            column,
            column,
            self.send_plane.at[flip - 1],
            self.recv_plane.at[flip - 1],
            fsdp=jnp.bitwise_xor(self.place.plane, flip),
        )

    def second(self, flip):
        origin = jnp.bitwise_xor(self.place.plane, flip)
        part = self.whole.at[pl.ds((flip - 1) * self.half, self.half), origin]
        return remote(
            part,
            part,
            self.send_plane.at[flip + 1],
            self.recv_plane.at[flip + 1],
            fsdp=jnp.bitwise_xor(self.place.plane, 3 - flip),
        )

    def spread(self):
        self.own(False).wait()
        for step in range(1, self.place.ranks):
            self.piece(step).wait()
        for flip in (1, 2):
            self.first(flip).start()

    def relay(self):
        for flip in (1, 2):
            self.first(flip).wait_recv()
            self.second(flip).start()

    def finish(self):
        for flip in (1, 2):
            self.first(flip).wait_send()
            self.second(flip).wait()


def split(refs, *counts):
    groups, first = [], 0
    for count in counts:
        groups.append(refs[first : first + count])
        first += count
    return groups


HBM_SPEC = pl.BlockSpec(memory_space=pltpu.HBM)
VMEM_SPEC = pl.BlockSpec(memory_space=pltpu.VMEM)


def comm_call(body, number, outs, ins, scratch, args, flops=0, **more):
    return pl.pallas_call(
        body,
        out_shape=[shape for shape, spec in outs],
        in_specs=ins,
        out_specs=[spec for shape, spec in outs],
        scratch_shapes=scratch,
        compiler_params=pltpu.CompilerParams(
            collective_id=number, has_side_effects=True, vmem_limit_bytes=62 * 1024 * 1024
        ),
        **more,
    )(*args)


def front(ranks, planes, rows_in, attn_shard, gate_shard):
    rows, width = rows_in.shape
    deep, columns = attn_shard.shape[0], attn_shard.shape[1] // ranks
    wide = gate_shard.shape[1] // ranks

    def body(x, wa, wg, seq, attn, gate, *scratch):
        place = Place(ranks)
        for_seq, for_attn, for_gate = split(scratch, 3, 5, 5)
        gather = Gather(place, x, seq, *for_seq)
        attn_w = Exchange(place, wa, attn, *for_attn)
        gate_w = Exchange(place, wg, gate, *for_gate)
        place.greet(True, True)
        attn_w.start()
        gather.start()
        gather.relay(1)
        attn_w.spread()
        gate_w.start()
        gather.relay(2)
        gather.relay(3)
        attn_w.relay()
        gather.finish()
        attn_w.finish()
        gate_w.spread()
        gate_w.relay()
        gate_w.finish()

    low = jnp.bfloat16
    return comm_call(
        body,
        0,
        [
            (jax.ShapeDtypeStruct((ranks, rows, width), low), HBM_SPEC),
            (jax.ShapeDtypeStruct((ranks, planes, deep, columns), low), HBM_SPEC),
            (jax.ShapeDtypeStruct((ranks, planes, deep, wide), low), HBM_SPEC),
        ],
        [HBM_SPEC] * 3,
        Gather.scratch(ranks)
        + Exchange.scratch(ranks, deep, columns)
        + Exchange.scratch(ranks, deep, wide),
        (rows_in, attn_shard, gate_shard),
    )


def column_gather(number, ranks, planes, rows_in, shard=None):
    rows, width = rows_in.shape
    outs = [(jax.ShapeDtypeStruct((ranks, rows, width), jnp.bfloat16), HBM_SPEC)]
    scratch = Gather.scratch(ranks)
    args = [rows_in]
    if shard is not None:
        deep, wide = shard.shape[0], shard.shape[1] // ranks
        outs.append((jax.ShapeDtypeStruct((ranks, planes, deep, wide), jnp.bfloat16), HBM_SPEC))
        scratch = scratch + Exchange.scratch(ranks, deep, wide)
        args.append(shard)
    count = len(args)

    def body(*refs):
        ins, made, mine, rest = split(refs, count, count, 3, 5)
        place = Place(ranks)
        gather = Gather(place, ins[0], made[0], *mine)
        place.greet(shard is not None, shard is not None)
        if shard is not None:
            weight = Exchange(place, ins[1], made[1], *rest)
            weight.start()
        gather.start()
        gather.relay(1)
        if shard is not None:
            weight.spread()
        gather.relay(2)
        gather.relay(3)
        gather.finish()
        if shard is not None:
            weight.relay()
            weight.finish()

    return comm_call(body, number, outs, [HBM_SPEC] * count, scratch, args)


def column_scatter(number, ranks, planes, parts, shard=None):
    rows, width = parts.shape[0] // ranks, parts.shape[1]
    outs = [(jax.ShapeDtypeStruct((rows, width), jnp.float32), VMEM_SPEC)]
    scratch = Scatter.scratch(ranks, rows, width)
    args = [parts.reshape(ranks, rows, width)]
    ins = [VMEM_SPEC]
    if shard is not None:
        deep, wide = shard.shape[0], shard.shape[1] // ranks
        outs.append((jax.ShapeDtypeStruct((ranks, planes, deep, wide), jnp.bfloat16), HBM_SPEC))
        scratch = scratch + Exchange.scratch(ranks, deep, wide)
        args.append(shard)
        ins.append(HBM_SPEC)
    count = len(args)

    def body(*refs):
        given, made, mine, rest = split(refs, count, count, 6, 5)
        place = Place(ranks)
        scatter = Scatter(place, given[0], made[0], *mine)
        place.greet(shard is not None, shard is not None)
        scatter.start()
        if shard is not None:
            weight = Exchange(place, given[1], made[1], *rest)
            weight.start()
        scatter.run()
        scatter.finish()
        if shard is not None:
            weight.spread()
            weight.relay()
            weight.finish()

    return comm_call(body, number, outs, ins, scratch, args)


def weights_out(grads, ranks, planes):
    rows = grads.shape[0] // (ranks * planes)
    parted = grads.astype(jnp.bfloat16).reshape(ranks, planes, rows, grads.shape[1])
    parted = parted.transpose(1, 0, 2, 3).reshape(grads.shape)
    sums = lax.psum_scatter(parted, "fsdp", scatter_dimension=0, tiled=True)
    return lax.all_to_all(
        sums.reshape(ranks, rows, -1), "cp", split_axis=0, concat_axis=1, tiled=False
    )


def by_heads(
    tokens, gains, w_query, w_key, w_value, w_out, w_gate, w_up, w_down, order, cotangent
):
    width = tokens.shape[-1]
    span = tokens.shape[2]
    rows = w_query.shape[0]
    ranks = lax.axis_size("cp")
    planes = lax.axis_size("fsdp")
    scale_q = HEAD ** (-0.5)
    rank = lax.axis_index("cp")
    even = rank % 2 == 0
    offsets = jnp.arange(span, dtype=jnp.int32)
    positions = (order[:, None] * span + offsets[None, :]).reshape(-1)
    visible = positions[None, :] <= positions[:, None]
    inverse = jnp.exp(-math.log(ROPE_BASE) * jnp.arange(HEAD // 2, dtype=jnp.float32) * 2.0 / HEAD)
    angle = positions.astype(jnp.float32)[:, None] * inverse[None, :]
    cosine = jnp.cos(angle)
    sine = jnp.sin(angle)
    mixed_cos = jnp.where(even, cosine, 1.0)
    mixed_sin = jnp.where(even, sine, 0.0)

    def turn(values, cos_t, sin_t):
        middle = values.shape[-1] // 2
        first = values[:, :middle]
        second = values[:, middle:]
        return jnp.concatenate(
            [first * cos_t - second * sin_t, second * cos_t + first * sin_t], axis=-1
        )

    swap = [(i, i ^ 1) for i in range(ranks)]
    hidden = tokens.reshape(-1, width).astype(jnp.float32)
    normed_one, factor_one = normalize(hidden)
    attn_in = (normed_one * gains[0]).astype(jnp.bfloat16)
    pairs = jnp.stack(
        [w_key.reshape(rows, KV_HEADS, HEAD), w_value.reshape(rows, KV_HEADS, HEAD)], axis=2
    ).reshape(rows, ranks, HEAD)
    attn_shard = jnp.concatenate(
        [w_query.reshape(rows, ranks, HEAD), pairs, w_out.reshape(rows, ranks, HEAD)], axis=-1
    ).reshape(rows, -1)
    seq_in, attn_w, gate_part = front(ranks, planes, attn_in, attn_shard, w_gate)
    seq_in = seq_in.reshape(-1, width)
    attn_w = attn_w.reshape(width, -1)
    gate_part = gate_part.reshape(width, -1)
    w_lin = attn_w[:, : 2 * HEAD]
    w_back = attn_w[:, 2 * HEAD :]
    lin = jnp.dot(seq_in, w_lin, preferred_element_type=jnp.float32)
    query = turn(lin[:, :HEAD], cosine, sine).astype(jnp.bfloat16)
    mixed = turn(lin[:, HEAD:], mixed_cos, mixed_sin).astype(jnp.bfloat16)
    other = lax.ppermute(mixed, "cp", swap)
    keys = jnp.where(even, mixed, other)
    values = jnp.where(even, other, mixed)
    raw = lax.dot_general(query, keys, CONTRACT_LAST, preferred_element_type=jnp.float32) * scale_q
    bent = jnp.tanh(raw / SOFT_CAP)
    scores = jnp.where(visible, SOFT_CAP * bent, -1e30)
    top_score = jnp.max(scores, axis=-1, keepdims=True)
    expo = jnp.exp(scores - top_score)
    total_mass = jnp.sum(expo, axis=-1, keepdims=True)
    probs_full = expo / total_mass
    probs_low = probs_full.astype(jnp.bfloat16)
    attended_low = jnp.dot(probs_low, values, preferred_element_type=jnp.float32).astype(
        jnp.bfloat16
    )
    share_attn = lax.dot_general(
        attended_low, w_back, CONTRACT_LAST, preferred_element_type=jnp.float32
    )
    attn_out, up_part = column_scatter(1, ranks, planes, share_attn.astype(jnp.bfloat16), w_up)
    up_part = up_part.reshape(width, -1)
    normed_two, factor_two = normalize(attn_out)
    middle_sum = hidden + normed_two * gains[1]
    normed_three, factor_three = normalize(middle_sum)
    ffn_in = (normed_three * gains[2]).astype(jnp.bfloat16)
    group_in, down_part = column_gather(2, ranks, planes, ffn_in, w_down)
    group_in = group_in.reshape(-1, width)
    down_part = down_part.reshape(width, -1)
    gate = jnp.dot(group_in, gate_part, preferred_element_type=jnp.float32)
    upper = jnp.dot(group_in, up_part, preferred_element_type=jnp.float32)
    activated = jax.nn.gelu(gate, approximate=True)
    inner_low = (activated * upper).astype(jnp.bfloat16)
    share_out = lax.dot_general(
        inner_low, down_part, CONTRACT_LAST, preferred_element_type=jnp.float32
    )
    (ffn_out,) = column_scatter(3, ranks, planes, share_out.astype(jnp.bfloat16))
    normed_four, factor_four = normalize(ffn_out)
    result = middle_sum + normed_four * gains[3]
    output = result.astype(jnp.bfloat16).reshape(tokens.shape)
    grad_result = cotangent.reshape(-1, width).astype(jnp.float32)
    gain_four = jnp.sum(grad_result * normed_four, axis=0)
    grad_ffn_low = norm_back(grad_result * gains[3], normed_four, factor_four).astype(jnp.bfloat16)
    (group_grad,) = column_gather(4, ranks, planes, grad_ffn_low)
    group_grad = group_grad.reshape(-1, width)
    grad_inner = jnp.dot(group_grad, down_part, preferred_element_type=jnp.float32)
    unused_value, gelu_back = jax.vjp(partial(jax.nn.gelu, approximate=True), gate)
    grad_gate_low = gelu_back(grad_inner * upper)[0].astype(jnp.bfloat16)
    grad_upper_low = (grad_inner * activated).astype(jnp.bfloat16)
    share_in = lax.dot_general(
        grad_gate_low, gate_part, CONTRACT_LAST, preferred_element_type=jnp.float32
    ) + lax.dot_general(grad_upper_low, up_part, CONTRACT_LAST, preferred_element_type=jnp.float32)
    (grad_ffn_in,) = column_scatter(5, ranks, planes, share_in.astype(jnp.bfloat16))
    grad_gate, grad_up, grad_down = (
        weights_out(
            lax.dot_general(left, right, CONTRACT_FIRST, preferred_element_type=jnp.float32),
            ranks,
            planes,
        )
        .astype(jnp.float32)
        .reshape(rows, -1)
        for left, right in (
            (group_in, grad_gate_low),
            (group_in, grad_upper_low),
            (group_grad, inner_low),
        )
    )
    gain_three = jnp.sum(grad_ffn_in * normed_three, axis=0)
    grad_middle = grad_result + norm_back(grad_ffn_in * gains[2], normed_three, factor_three)
    gain_two = jnp.sum(grad_middle * normed_two, axis=0)
    grad_attn_low = norm_back(grad_middle * gains[1], normed_two, factor_two).astype(jnp.bfloat16)
    (seq_grad,) = column_gather(6, ranks, planes, grad_attn_low)
    seq_grad = seq_grad.reshape(-1, width)
    grad_att_low = jnp.dot(seq_grad, w_back, preferred_element_type=jnp.float32).astype(
        jnp.bfloat16
    )
    grad_probs = lax.dot_general(
        grad_att_low, values, CONTRACT_LAST, preferred_element_type=jnp.float32
    )
    delta = jnp.sum(grad_probs * probs_full, axis=-1, keepdims=True)
    grad_raw = (probs_full * (grad_probs - delta) * (1.0 - bent * bent)).astype(jnp.bfloat16)
    grad_query = jnp.dot(grad_raw, keys, preferred_element_type=jnp.float32) * scale_q
    grad_keys = (
        lax.dot_general(grad_raw, query, CONTRACT_FIRST, preferred_element_type=jnp.float32)
        * scale_q
    )
    grad_values = lax.dot_general(
        probs_low, grad_att_low, CONTRACT_FIRST, preferred_element_type=jnp.float32
    )
    grad_mixed = jnp.where(even, grad_keys, grad_values) + lax.ppermute(
        jnp.where(even, grad_values, grad_keys), "cp", swap
    )
    grad_lin = jnp.concatenate(
        [
            turn(grad_query, cosine, -sine).astype(jnp.bfloat16),
            turn(grad_mixed, mixed_cos, -mixed_sin).astype(jnp.bfloat16),
        ],
        axis=1,
    )
    share_back = lax.dot_general(
        grad_lin, w_lin, CONTRACT_LAST, preferred_element_type=jnp.float32
    )
    (grad_attn_in,) = column_scatter(7, ranks, planes, share_back.astype(jnp.bfloat16))
    attn_sums = weights_out(
        jnp.concatenate(
            [
                lax.dot_general(
                    seq_in, grad_lin, CONTRACT_FIRST, preferred_element_type=jnp.float32
                ),
                lax.dot_general(
                    seq_grad, attended_low, CONTRACT_FIRST, preferred_element_type=jnp.float32
                ),
            ],
            axis=1,
        ),
        ranks,
        planes,
    ).astype(jnp.float32)
    grad_wq = attn_sums[:, :, :HEAD].reshape(rows, -1)
    grad_pairs = attn_sums[:, :, HEAD : 2 * HEAD].reshape(rows, KV_HEADS, 2, HEAD)
    grad_wk = grad_pairs[:, :, 0].reshape(rows, -1)
    grad_wv = grad_pairs[:, :, 1].reshape(rows, -1)
    grad_wo = attn_sums[:, :, 2 * HEAD :].reshape(rows, -1)
    gain_one = jnp.sum(grad_attn_in * normed_one, axis=0)
    grad_hidden = grad_middle + norm_back(grad_attn_in * gains[0], normed_one, factor_one)
    gain_columns = jnp.stack([gain_one, gain_two, gain_three, gain_four], axis=1)
    grad_gains = lax.psum_scatter(
        gain_columns, ("cp", "fsdp"), scatter_dimension=0, tiled=True
    ).T
    return (
        output,
        grad_hidden.reshape(tokens.shape),
        grad_gains,
        grad_wq,
        grad_wk,
        grad_wv,
        grad_wo,
        grad_gate,
        grad_up,
        grad_down,
    )


def solution(mesh):
    return jax.shard_map(
        by_heads if mesh.shape["cp"] == HEADS else local,
        mesh=mesh,
        in_specs=(
            P("fsdp", "cp", None, None),
            P(),
            P(("cp", "fsdp"), None),
            P(("cp", "fsdp"), None),
            P(("cp", "fsdp"), None),
            P(("cp", "fsdp"), None),
            P(("cp", "fsdp"), None),
            P(("cp", "fsdp"), None),
            P(("cp", "fsdp"), None),
            P(),
            P("fsdp", "cp", None, None),
        ),
        out_specs=(
            P("fsdp", "cp", None, None),
            P("fsdp", "cp", None, None),
            P(None, ("cp", "fsdp")),
            P(("cp", "fsdp"), None),
            P(("cp", "fsdp"), None),
            P(("cp", "fsdp"), None),
            P(("cp", "fsdp"), None),
            P(("cp", "fsdp"), None),
            P(("cp", "fsdp"), None),
            P(("cp", "fsdp"), None),
        ),
        check_vma=False,
    )
```
